32 devices in a mesh: sys: 4 (over y, z), seg: 8 (over x, core).
Axes of the slice: x: 4, y: 2, z: 2, core: 2. Of those that a mesh axis runs over, the one named last changes fastest.
The devices are a block of a 4x4x8 slice.
Arguments:
- positions: bfloat16 [98304, 512], P(('sys', 'seg')), parts along dimension 0
- charges: float32 [98304], P(('sys', 'seg')), parts along dimension 0
- pair_band: int32 [32, 7], P(('sys', 'seg')), parts along dimension 0
Outputs:
- output 1: float32 [98304, 512], P(('sys', 'seg')), parts along dimension 0
- output 2: float32 [4], P('sys'), parts along dimension 0
There are 4 independent parts. The reference program is written for one: setup_inputs(seed, part) draws one part's arguments, and reference() takes and returns one part's arrays. A program takes and returns all parts, laid end to end along the dimension named above; each array names one.
All inputs are finite; a program needn't handle non-finite values.
Results may differ from the reference program's by a relative error of at most 0.001.
Values are sent between devices in bfloat16 or wider.
A program may use at most 768 MiB of HBM per device.

```python
import jax
import jax.numpy as jnp
from jax import lax

SEG_COUNT = 8
BLOCK_ROWS = 3072
FEAT_DIM = 512
REACH_STEPS = 3


def draw_band(mask_key):
    coin_draw = jax.random.randint(mask_key, (SEG_COUNT, REACH_STEPS), 0, 3)
    block_ids = jnp.arange(SEG_COUNT)[:, None]
    step_ids = jnp.arange(REACH_STEPS)[None, :]
    upper_cols = jnp.where((block_ids == 0) & (step_ids == REACH_STEPS - 1), 1, (coin_draw > 0).astype(jnp.int32))
    lower_list = [jnp.roll(upper_cols[:, step_idx - 1], step_idx) for step_idx in range(REACH_STEPS, 0, -1)]
    higher_list = [upper_cols[:, step_idx - 1] for step_idx in range(1, REACH_STEPS + 1)]
    centre_list = [jnp.ones((SEG_COUNT,), jnp.int32)]
    return jnp.stack(lower_list + centre_list + higher_list, axis=1).astype(jnp.int32)


def setup_inputs(seed: int = 0, part: int = 0) -> dict:
    part_key = jax.random.fold_in(jax.random.key(seed), part)
    pos_key, sign_key, mag_key, mask_key = jax.random.split(part_key, 4)
    all_rows = SEG_COUNT * BLOCK_ROWS
    pos_vals = jax.random.normal(pos_key, (all_rows, FEAT_DIM), jnp.float32)
    sign_vals = 2.0 * jax.random.randint(sign_key, (all_rows,), 0, 2).astype(jnp.float32) - 1.0
    magnitude = jax.random.uniform(mag_key, (all_rows,), jnp.float32, 0.5, 1.5)
    charge_scale = FEAT_DIM ** 0.5 * (BLOCK_ROWS * (2 * REACH_STEPS + 1)) ** -0.25
    return {'positions': pos_vals.astype(jnp.bfloat16), 'charges': sign_vals * magnitude * charge_scale, 'pair_band': draw_band(mask_key)}


def reference(positions, charges, pair_band):
    inv_lsq = 1.0 / FEAT_DIM
    pos_blocks = positions.reshape(SEG_COUNT, BLOCK_ROWS, FEAT_DIM)
    charge_blocks = charges.reshape(SEG_COUNT, BLOCK_ROWS)
    row_ids = jnp.arange(BLOCK_ROWS)
    self_pair = row_ids[:, None] == row_ids[None, :]
    offsets = jnp.arange(-REACH_STEPS, REACH_STEPS + 1)

    def one_block(host_blk):
        x_host = pos_blocks[host_blk]
        host_f32 = x_host.astype(jnp.float32)
        host_sq = jnp.sum(host_f32 * host_f32, axis=1)
        q_host = charge_blocks[host_blk]

        def one_offset(carry_state, offset):
            force_acc, energy_acc = carry_state
            other_blk = (host_blk + offset) % SEG_COUNT
            x_other = pos_blocks[other_blk]
            other_f32 = x_other.astype(jnp.float32)
            other_sq = jnp.sum(other_f32 * other_f32, axis=1)
            cross_dot = jnp.dot(x_host, x_other.T, preferred_element_type=jnp.float32)
            sq_dist = jnp.maximum(host_sq[:, None] + other_sq[None, :] - 2.0 * cross_dot, 0.0)
            weights = q_host[:, None] * charge_blocks[other_blk][None, :] * jnp.exp(sq_dist * (-0.5 * inv_lsq))
            keep_pair = (pair_band[host_blk, REACH_STEPS + offset] != 0) & jnp.logical_not(self_pair & (offset == 0))
            weights = jnp.where(keep_pair, weights, 0.0)
            pull_term = jnp.dot(weights.astype(jnp.bfloat16), x_other, preferred_element_type=jnp.float32)
            force_acc = force_acc + (jnp.sum(weights, axis=1)[:, None] * host_f32 - pull_term) * inv_lsq
            energy_acc = energy_acc + 0.5 * jnp.sum(weights)
            return (force_acc, energy_acc), None

        init_carry = (jnp.zeros((BLOCK_ROWS, FEAT_DIM), jnp.float32), jnp.zeros((), jnp.float32))
        (force_blk, energy_blk), _ = lax.scan(one_offset, init_carry, offsets)
        return force_blk, energy_blk

    force_blocks, block_energy = lax.map(one_block, jnp.arange(SEG_COUNT))
    return force_blocks.reshape(SEG_COUNT * BLOCK_ROWS, FEAT_DIM), jnp.sum(block_energy).reshape(1)
```

```python
import functools
import math

import jax
import jax.numpy as jnp
from jax import lax
from jax.experimental import pallas as pl
from jax.experimental.pallas import tpu as pltpu
from jax.sharding import PartitionSpec as P

MESH = pl.DeviceIdType.MESH
LANES = 128
CHUNKS = 6
ROW_TILE = 1024


def kernel(seg_len, reach, band_ref, x_hbm, q_ref, f_hbm, e_ref, x_all, meta, a_col, q_col, acc, row_acc, e_buf,
           local_sem, send_sem, recv_sem, msend_sem, mrecv_sem, esend_sem, erecv_sem, out_sem):
    n, d = x_hbm.shape
    chunk = n // CHUNKS
    me = lax.axis_index('seg')
    core = lax.rem(me, 2)
    mate = me + 1 - 2 * core
    right = lax.rem(me + 2, seg_len)
    left = lax.rem(me + seg_len - 2, seg_len)
    right_x = right + 1 - 2 * core
    left_x = left + 1 - 2 * core
    far_x = lax.rem(me + 4, seg_len) + 1 - 2 * core
    scale = math.log2(math.e) * 0.5 / d
    inv_lsq = 1.0 / d

    load = pltpu.make_async_copy(x_hbm, x_all.at[0], local_sem)
    load.start()

    barrier = pltpu.get_barrier_semaphore()
    for hop in range(1, seg_len):
        pl.semaphore_signal(barrier, inc=1, device_id={'seg': lax.rem(me + hop, seg_len)}, device_id_type=MESH)
    pl.semaphore_wait(barrier, seg_len - 1)

    def send(kind, k, src, slot, dev):
        rows = pl.ds(pl.multiple_of(k * chunk, chunk), chunk)
        return pltpu.make_async_remote_copy(
            src_ref=src.at[rows], dst_ref=x_all.at[slot, rows], send_sem=send_sem.at[kind, k],
            recv_sem=recv_sem.at[slot, k], device_id={'seg': dev}, device_id_type=MESH)

    def to_right(k):
        return send(0, k, x_hbm, 1, right)

    def to_left(k):
        return send(1, k, x_hbm, 2, left)

    def to_mate(k):
        return send(2, k, x_hbm, 6, mate)

    def pass_left_block(k):
        return send(3, k, x_all.at[1], 3, mate)

    def pass_right_block(k):
        return send(4, k, x_all.at[2], 4, mate)

    def pass_far(k):
        onward = core * right_x + (1 - core) * left_x
        return send(5, k, x_all.at[2 - core], 5, onward)

    to_right(0).start()
    to_left(0).start()
    load.wait()

    def prologue(r, _):
        rows = pl.ds(pl.multiple_of(r * LANES, LANES), LANES)
        x = x_all[0, rows, :].astype(jnp.float32)
        neg = jnp.sum(x * x, axis=1, keepdims=True) * (-scale)
        neg = jnp.broadcast_to(neg, (LANES, LANES))
        a_col[rows, :] = neg
        q_row = q_ref[:, rows]
        meta[0, 1:2, rows] = neg.T[0:1, :]
        meta[0, 0:1, rows] = q_row
        q_col[rows, :] = jnp.broadcast_to(q_row, (LANES, LANES)).T
        row_acc[rows, :] = jnp.zeros((LANES, LANES), jnp.float32)
        acc[rows, :] = jnp.zeros((LANES, d), jnp.float32)
        return 0

    lax.fori_loop(0, n // LANES, prologue, 0)

    to_mate(0).start()
    peers = ((1, right), (2, left), (3, right_x), (4, left_x), (5, far_x), (6, mate))
    metas = [
        pltpu.make_async_remote_copy(
            src_ref=meta.at[0], dst_ref=meta.at[slot], send_sem=msend_sem.at[slot], recv_sem=mrecv_sem.at[slot],
            device_id={'seg': dev}, device_id_type=MESH)
        for slot, dev in peers]
    for copy in metas:
        copy.start()

    def start_rest(k, _):
        to_right(k).start()
        to_left(k).start()
        to_mate(k).start()
        return 0

    lax.fori_loop(1, CHUNKS, start_rest, 0)

    def block_part(slot, k, column, own):
        cols = pl.ds(pl.multiple_of(k * chunk, chunk), chunk)
        live = band_ref[0, column] != 0
        q_row = jnp.where(live, meta[slot, 0:1, cols], 0.0)
        b_row = meta[slot, 1:2, cols]

        def row_tile(i, _):
            rows = pl.ds(pl.multiple_of(i * ROW_TILE, ROW_TILE), ROW_TILE)
            x_vis = x_all[slot, cols, :]
            dots = lax.dot_general(x_all[0, rows, :], x_vis, (((1,), (1,)), ((), ())),
                                   preferred_element_type=jnp.float32)
            a_tile = jnp.concatenate([a_col[rows, :]] * (chunk // LANES), axis=1)
            q_tile = jnp.concatenate([q_col[rows, :]] * (chunk // LANES), axis=1)
            weights = jnp.exp2(jnp.minimum((dots * (2.0 * scale) + a_tile) + b_row, 0.0)) * q_row * q_tile
            if own:
                row_id = lax.broadcasted_iota(jnp.int32, weights.shape, 0) + i * ROW_TILE
                col_id = lax.broadcasted_iota(jnp.int32, weights.shape, 1) + k * chunk
                weights = jnp.where(row_id == col_id, 0.0, weights)
            part = weights[:, 0:LANES]
            for s in range(1, chunk // LANES):
                part = part + weights[:, s * LANES:(s + 1) * LANES]
            row_acc[rows, :] += part
            acc[rows, :] += jnp.dot(weights.astype(jnp.bfloat16), x_vis, preferred_element_type=jnp.float32)
            return 0

        lax.fori_loop(0, n // ROW_TILE, row_tile, 0)

    def serve(k):
        to_right(k).wait_recv()
        to_left(k).wait_recv()
        pass_left_block(k).start()
        pass_right_block(k).start()
        pass_far(k).start()

    def own_part(k, _):
        block_part(0, k, reach, True)
        return 0

    lax.fori_loop(0, CHUNKS, own_part, 0)
    serve(0)
    for copy in metas:
        copy.wait_recv()

    def mate_part(k, _):
        to_mate(k).wait_recv()
        block_part(6, k, reach + 1 - 2 * core, False)
        return 0

    lax.fori_loop(0, CHUNKS, mate_part, 0)

    def ring_round(k, _):
        @pl.when(k + 1 < CHUNKS)
        def _():
            serve(k + 1)

        pass_left_block(k).wait_recv()
        pass_right_block(k).wait_recv()

        def ring_part(slot, _):
            direct = jnp.where(slot == 1, reach - 2, reach + 2)
            crossed = jnp.where(slot == 3, reach - 1 - 2 * core, reach + 3 - 2 * core)
            block_part(slot, k, jnp.where(slot < 3, direct, crossed), False)
            return 0

        lax.fori_loop(1, 5, ring_part, 0)
        return 0

    lax.fori_loop(0, CHUNKS, ring_round, 0)

    def far_part(k, _):
        pass_far(k).wait_recv()
        block_part(5, k, 2 * reach * core, False)
        return 0

    lax.fori_loop(0, CHUNKS, far_part, 0)

    total = jnp.zeros((8, LANES), jnp.float32)

    def add_rows(r, total):
        rows = pl.ds(pl.multiple_of(r * LANES, LANES), LANES)
        return total + jnp.sum(row_acc[rows, :].reshape(LANES // 8, 8, LANES), axis=0)

    total = lax.fori_loop(0, n // LANES, add_rows, total)
    e_buf[me] = jnp.broadcast_to(0.5 * jnp.sum(total), (8, LANES))

    def finish(r, _):
        rows = pl.ds(pl.multiple_of(r * LANES, LANES), LANES)
        row_sum = jnp.sum(row_acc[rows, :], axis=1, keepdims=True)
        acc[rows, :] = (row_sum * x_all[0, rows, :].astype(jnp.float32) - acc[rows, :]) * inv_lsq
        return 0

    def out_copy(r):
        rows = pl.ds(pl.multiple_of(r * LANES, LANES), LANES)
        return pltpu.make_async_copy(acc.at[rows], f_hbm.at[rows], out_sem.at[r])

    finish(0, 0)
    energy = [
        pltpu.make_async_remote_copy(
            src_ref=e_buf.at[me], dst_ref=e_buf.at[me], send_sem=esend_sem.at[hop], recv_sem=erecv_sem.at[hop],
            device_id={'seg': lax.rem(me + hop, seg_len)}, device_id_type=MESH)
        for hop in range(1, seg_len)]
    for copy in energy:
        copy.start()

    def finish_and_send(r, _):
        finish(r, 0)
        out_copy(r - 1).start()
        return 0

    lax.fori_loop(1, n // LANES, finish_and_send, 0)
    out_copy(n // LANES - 1).start()

    def drain(k, _):
        for copy in (to_right, to_left, to_mate, pass_left_block, pass_right_block, pass_far):
            copy(k).wait_send()
        return 0

    lax.fori_loop(0, CHUNKS, drain, 0)
    for copy in metas:
        copy.wait_send()
    for copy in energy:
        copy.wait()
    e_sum = e_buf[0]
    for dev in range(1, seg_len):
        e_sum = e_sum + e_buf[dev]
    e_ref[...] = e_sum

    def drain_out(r, _):
        out_copy(r).wait()
        return 0

    lax.fori_loop(0, n // LANES, drain_out, 0)


def solution(mesh):
    seg_len = mesh.shape['seg']

    def device_fn(positions, charges, pair_band):
        n, d = positions.shape
        reach = (pair_band.shape[1] - 1) // 2
        flops = 4 * n * n * d * (2 * reach + 1)
        forces, energy = pl.pallas_call(
            functools.partial(kernel, seg_len, reach),
            out_shape=(jax.ShapeDtypeStruct((n, d), jnp.float32), jax.ShapeDtypeStruct((8, LANES), jnp.float32)),
            in_specs=[pl.BlockSpec(memory_space=pltpu.SMEM), pl.BlockSpec(memory_space=pl.ANY),
                      pl.BlockSpec(memory_space=pltpu.VMEM)],
            out_specs=(pl.BlockSpec(memory_space=pl.ANY), pl.BlockSpec(memory_space=pltpu.VMEM)),
            scratch_shapes=[
                pltpu.VMEM((7, n, d), jnp.bfloat16),
                pltpu.VMEM((7, 2, n), jnp.float32),
                pltpu.VMEM((n, LANES), jnp.float32),
                pltpu.VMEM((n, LANES), jnp.float32),
                pltpu.VMEM((n, d), jnp.float32),
                pltpu.VMEM((n, LANES), jnp.float32),
                pltpu.VMEM((seg_len, 8, LANES), jnp.float32),
                pltpu.SemaphoreType.DMA,
                pltpu.SemaphoreType.DMA((6, CHUNKS)),
                pltpu.SemaphoreType.DMA((7, CHUNKS)),
                pltpu.SemaphoreType.DMA((7,)),
                pltpu.SemaphoreType.DMA((7,)),
                pltpu.SemaphoreType.DMA((seg_len,)),
                pltpu.SemaphoreType.DMA((seg_len,)),
                pltpu.SemaphoreType.DMA((n // LANES,)),
            ],
            compiler_params=pltpu.CompilerParams(
                collective_id=0, has_side_effects=True, vmem_limit_bytes=60 * 2**20),
            cost_estimate=pl.CostEstimate(flops=flops, bytes_accessed=16 * n * d, transcendentals=0),
            name='pair_forces',
        )(pair_band, positions, charges.reshape(1, n))
        return forces, energy[0, 0].reshape(1)

    row_spec = P(('sys', 'seg'), None)
    vec_spec = P(('sys', 'seg'))
    return jax.shard_map(device_fn, mesh=mesh, in_specs=(row_spec, vec_spec, row_spec), out_specs=(row_spec, P('sys')), check_vma=False)
```

```python
import functools
import math

import jax
import jax.numpy as jnp
from jax import lax
from jax.experimental import pallas as pl
from jax.experimental.pallas import tpu as pltpu
from jax.sharding import PartitionSpec as P

MESH = pl.DeviceIdType.MESH
LANES = 128
CHUNKS = 6
TILE = 256
PIECE = 64


def kernel(seg_len, reach, band_ref, x_hbm, q_ref, f_hbm, e_ref, x_all, meta, a_col, q_col, acc, row_acc, s_buf, w_buf, diag, e_buf,
           local_sem, send_sem, recv_sem, msend_sem, mrecv_sem, esend_sem, erecv_sem, out_sem):
    n, d = x_hbm.shape
    chunk = n // CHUNKS
    me = lax.axis_index('seg')
    core = lax.rem(me, 2)
    mate = me + 1 - 2 * core
    right = lax.rem(me + 2, seg_len)
    left = lax.rem(me + seg_len - 2, seg_len)
    right_x = right + 1 - 2 * core
    left_x = left + 1 - 2 * core
    far_x = lax.rem(me + 4, seg_len) + 1 - 2 * core
    scale = math.log2(math.e) * 0.5 / d
    inv_lsq = 1.0 / d

    load = pltpu.make_async_copy(x_hbm, x_all.at[0], local_sem)
    load.start()

    barrier = pltpu.get_barrier_semaphore()
    for hop in range(1, seg_len):
        pl.semaphore_signal(barrier, inc=1, device_id={'seg': lax.rem(me + hop, seg_len)}, device_id_type=MESH)
    pl.semaphore_wait(barrier, seg_len - 1)

    def send(kind, k, src, slot, dev):
        rows = pl.ds(pl.multiple_of(k * chunk, chunk), chunk)
        return pltpu.make_async_remote_copy(
            src_ref=src.at[rows], dst_ref=x_all.at[slot, rows], send_sem=send_sem.at[kind, k],
            recv_sem=recv_sem.at[slot, k], device_id={'seg': dev}, device_id_type=MESH)

    def to_right(k):
        return send(0, k, x_hbm, 1, right)

    def to_left(k):
        return send(1, k, x_hbm, 2, left)

    def to_mate(k):
        return send(2, k, x_hbm, 6, mate)

    def pass_left_block(k):
        return send(3, k, x_all.at[1], 3, mate)

    def pass_right_block(k):
        return send(4, k, x_all.at[2], 4, mate)

    def pass_far(k):
        onward = core * right_x + (1 - core) * left_x
        return send(5, k, x_all.at[2 - core], 5, onward)

    to_right(0).start()
    to_left(0).start()
    load.wait()

    def prologue(r, _):
        rows = pl.ds(pl.multiple_of(r * LANES, LANES), LANES)
        x = x_all[0, rows, :].astype(jnp.float32)
        neg = jnp.sum(x * x, axis=1, keepdims=True) * (-scale)
        neg = jnp.broadcast_to(neg, (LANES, LANES))
        a_col[rows, :] = neg
        q_row = q_ref[:, rows]
        meta[0, 1:2, rows] = neg.T[0:1, :]
        meta[0, 0:1, rows] = q_row
        q_col[rows, :] = jnp.broadcast_to(q_row, (LANES, LANES)).T
        row_acc[rows, :] = jnp.zeros((LANES, LANES), jnp.float32)
        acc[rows, :] = jnp.zeros((LANES, d), jnp.float32)
        return 0

    lax.fori_loop(0, n // LANES, prologue, 0)

    to_mate(0).start()
    peers = ((1, right), (2, left), (3, right_x), (4, left_x), (5, far_x), (6, mate))
    metas = [
        pltpu.make_async_remote_copy(
            src_ref=meta.at[0], dst_ref=meta.at[slot], send_sem=msend_sem.at[slot], recv_sem=mrecv_sem.at[slot],
            device_id={'seg': dev}, device_id_type=MESH)
        for slot, dev in peers]
    for copy in metas:
        copy.start()
    columns = {1: reach - 2, 2: reach + 2, 3: reach - 1 - 2 * core, 4: reach + 3 - 2 * core, 5: 2 * reach * core,
               6: reach + 1 - 2 * core}

    def start_rest(k, _):
        to_right(k).start()
        to_left(k).start()
        to_mate(k).start()
        return 0

    lax.fori_loop(1, CHUNKS, start_rest, 0)

    meta[7] = jnp.zeros((2, n), jnp.float32)
    row_id = lax.broadcasted_iota(jnp.int32, (TILE, 2 * TILE), 0)
    col_id = lax.broadcasted_iota(jnp.int32, (TILE, 2 * TILE), 1)
    for half in range(2):
        diag[half] = jnp.where(row_id + half * TILE == col_id, -1e30, 0.0)
    diag[2] = jnp.zeros((TILE, 2 * TILE), jnp.float32)

    def serve(k):
        to_right(k).wait_recv()
        to_left(k).wait_recv()
        pass_left_block(k).start()
        pass_right_block(k).start()
        pass_far(k).start()

    tiles = n // TILE
    ring = 2 * CHUNKS
    last = ring + 4 * CHUNKS

    def place(task):
        turn = task - ring
        slot = jnp.where(task < CHUNKS, 0, jnp.where(task < ring, 6, jnp.where(task < last, 1 + lax.rem(turn, 4), 5)))
        k = jnp.where(task < CHUNKS, CHUNKS - 1 - task,
                      jnp.where(task < ring, task - CHUNKS, jnp.where(task < last, turn // 4, task - last)))
        return slot, k

    def block(slot, k):
        return x_all[slot, pl.ds(pl.multiple_of(k * chunk, chunk), chunk), :]

    def dots(i, slot, k):
        return lax.dot_general(x_all[0, i * TILE:(i + 1) * TILE, :], block(slot, k), (((1,), (1,)), ((), ())),
                               preferred_element_type=jnp.float32)

    def weigh(dot_tile, i, slot, k, buf, cap):
        for p in range(TILE // PIECE):
            rows = slice(i * TILE + p * PIECE, i * TILE + (p + 1) * PIECE)
            tile_rows = slice(p * PIECE, (p + 1) * PIECE)
            a_piece = a_col[rows, :]
            q_piece = q_col[rows, :]
            part = row_acc[rows, :]
            for h in range(chunk // LANES):
                lanes = slice(h * LANES, (h + 1) * LANES)
                cols = pl.ds(pl.multiple_of(k * chunk + h * LANES, LANES), LANES)
                power = (dot_tile[tile_rows, lanes] * (2.0 * scale) + a_piece) + meta[slot, 1:2, cols]
                power = jnp.minimum(power, 0.0 if cap is None else diag[cap, tile_rows, lanes])
                w = jnp.exp2(power) * meta[slot, 0:1, cols] * q_piece
                part = part + w
                w_buf[buf, tile_rows, lanes] = w.astype(jnp.bfloat16)
            row_acc[rows, :] = part

    def pull(i, slot, k, buf):
        acc[i * TILE:(i + 1) * TILE, :] += jnp.dot(w_buf[buf], block(slot, k), preferred_element_type=jnp.float32)

    def run_task(task, own):
        slot, k = place(task)
        was_slot, was_k = place(jnp.maximum(task - 1, 0))
        was_meta = jnp.where(task == 0, 7, was_slot)
        held = s_buf[...]
        for i in range(tiles):
            i1, slot1, k1, meta1 = (tiles - 1, was_slot, was_k, was_meta) if i == 0 else (i - 1, slot, k, slot)
            cap = None
            if own:
                step = i1 - 2 * k1
                cap = jnp.where((step == 0) | (step == 1), step, 2)
            fresh = dots(i, slot, k)
            weigh(held, i1, meta1, k1, i % 2, cap)
            pull(i1, slot1, k1, i % 2)
            held = fresh
        s_buf[...] = held

    s_buf[...] = jnp.zeros(s_buf.shape, jnp.float32)

    def own_task(task, _):
        @pl.when(task == CHUNKS - 1)
        def _():
            for copy in metas:
                copy.wait_recv()
            for s, column in columns.items():
                meta[s, 0:1, :] = jnp.where(band_ref[0, column] != 0, meta[s, 0:1, :], 0.0)

            def wait_mate(k, _):
                to_mate(k).wait_recv()
                return 0

            lax.fori_loop(0, CHUNKS, wait_mate, 0)
            serve(0)

        run_task(task, True)
        return 0

    lax.fori_loop(0, CHUNKS, own_task, 0)

    def other_task(task, _):
        coming = task + 1 - ring
        k = coming // 4

        @pl.when((coming >= 0) & (lax.rem(coming, 4) == 0) & (k < CHUNKS))
        def _():
            pass_left_block(k).wait_recv()
            pass_right_block(k).wait_recv()

            @pl.when(k + 1 < CHUNKS)
            def _():
                serve(k + 1)

        @pl.when((task + 1 >= last) & (task + 1 < last + CHUNKS))
        def _():
            pass_far(task + 1 - last).wait_recv()

        run_task(task, False)
        return 0

    lax.fori_loop(CHUNKS, last + CHUNKS, other_task, 0)

    slot, k = place(last + CHUNKS - 1)
    weigh(s_buf[...], tiles - 1, slot, k, 0, None)
    pull(tiles - 1, slot, k, 0)

    total = jnp.zeros((8, LANES), jnp.float32)

    def add_rows(r, total):
        rows = pl.ds(pl.multiple_of(r * LANES, LANES), LANES)
        return total + jnp.sum(row_acc[rows, :].reshape(LANES // 8, 8, LANES), axis=0)

    total = lax.fori_loop(0, n // LANES, add_rows, total)
    e_buf[me] = jnp.broadcast_to(0.5 * jnp.sum(total), (8, LANES))

    def finish(r, _):
        rows = pl.ds(pl.multiple_of(r * LANES, LANES), LANES)
        row_sum = jnp.sum(row_acc[rows, :], axis=1, keepdims=True)
        acc[rows, :] = (row_sum * x_all[0, rows, :].astype(jnp.float32) - acc[rows, :]) * inv_lsq
        return 0

    def out_copy(r):
        rows = pl.ds(pl.multiple_of(r * LANES, LANES), LANES)
        return pltpu.make_async_copy(acc.at[rows], f_hbm.at[rows], out_sem.at[r])

    finish(0, 0)
    energy = [
        pltpu.make_async_remote_copy(
            src_ref=e_buf.at[me], dst_ref=e_buf.at[me], send_sem=esend_sem.at[hop], recv_sem=erecv_sem.at[hop],
            device_id={'seg': lax.rem(me + hop, seg_len)}, device_id_type=MESH)
        for hop in range(1, seg_len)]
    for copy in energy:
        copy.start()

    def finish_and_send(r, _):
        finish(r, 0)
        out_copy(r - 1).start()
        return 0

    lax.fori_loop(1, n // LANES, finish_and_send, 0)
    out_copy(n // LANES - 1).start()

    def drain(k, _):
        for copy in (to_right, to_left, to_mate, pass_left_block, pass_right_block, pass_far):
            copy(k).wait_send()
        return 0

    lax.fori_loop(0, CHUNKS, drain, 0)
    for copy in metas:
        copy.wait_send()
    for copy in energy:
        copy.wait()
    e_sum = e_buf[0]
    for dev in range(1, seg_len):
        e_sum = e_sum + e_buf[dev]
    e_ref[...] = e_sum

    def drain_out(r, _):
        out_copy(r).wait()
        return 0

    lax.fori_loop(0, n // LANES, drain_out, 0)


def solution(mesh):
    seg_len = mesh.shape['seg']

    def device_fn(positions, charges, pair_band):
        n, d = positions.shape
        reach = (pair_band.shape[1] - 1) // 2
        flops = 4 * n * n * d * (2 * reach + 1)
        forces, energy = pl.pallas_call(
            functools.partial(kernel, seg_len, reach),
            out_shape=(jax.ShapeDtypeStruct((n, d), jnp.float32), jax.ShapeDtypeStruct((8, LANES), jnp.float32)),
            in_specs=[pl.BlockSpec(memory_space=pltpu.SMEM), pl.BlockSpec(memory_space=pl.ANY),
                      pl.BlockSpec(memory_space=pltpu.VMEM)],
            out_specs=(pl.BlockSpec(memory_space=pl.ANY), pl.BlockSpec(memory_space=pltpu.VMEM)),
            scratch_shapes=[
                pltpu.VMEM((7, n, d), jnp.bfloat16),
                pltpu.VMEM((8, 2, n), jnp.float32),
                pltpu.VMEM((n, LANES), jnp.float32),
                pltpu.VMEM((n, LANES), jnp.float32),
                pltpu.VMEM((n, d), jnp.float32),
                pltpu.VMEM((n, LANES), jnp.float32),
                pltpu.VMEM((TILE, 2 * TILE), jnp.float32),
                pltpu.VMEM((2, TILE, 2 * TILE), jnp.bfloat16),
                pltpu.VMEM((3, TILE, 2 * TILE), jnp.float32),
                pltpu.VMEM((seg_len, 8, LANES), jnp.float32),
                pltpu.SemaphoreType.DMA,
                pltpu.SemaphoreType.DMA((6, CHUNKS)),
                pltpu.SemaphoreType.DMA((7, CHUNKS)),
                pltpu.SemaphoreType.DMA((7,)),
                pltpu.SemaphoreType.DMA((7,)),
                pltpu.SemaphoreType.DMA((seg_len,)),
                pltpu.SemaphoreType.DMA((seg_len,)),
                pltpu.SemaphoreType.DMA((n // LANES,)),
            ],
            compiler_params=pltpu.CompilerParams(
                collective_id=0, has_side_effects=True, vmem_limit_bytes=60 * 2**20),
            cost_estimate=pl.CostEstimate(flops=flops, bytes_accessed=16 * n * d, transcendentals=0),
            name='pair_forces',
        )(pair_band, positions, charges.reshape(1, n))
        return forces, energy[0, 0].reshape(1)

    row_spec = P(('sys', 'seg'), None)
    vec_spec = P(('sys', 'seg'))
    return jax.shard_map(device_fn, mesh=mesh, in_specs=(row_spec, vec_spec, row_spec), out_specs=(row_spec, P('sys')), check_vma=False)
```

```python
import functools
import math

import jax
import jax.numpy as jnp
from jax import lax
from jax.experimental import pallas as pl
from jax.experimental.pallas import tpu as pltpu
from jax.sharding import PartitionSpec as P

MESH = pl.DeviceIdType.MESH
LANES = 128
CHUNKS = 6
TILE = 256
PIECE = 64
PIECES = TILE // PIECE
UNROLL = 2
SERVE = (0, 8, 10, 13, 15)


def gather_kernel(seg_len, reach, band_ref, x_hbm, q_ref, acc_hbm, row_hbm, a_hbm, q_hbm, meta_hbm, left_hbm, right_hbm,
                  left_x_hbm, right_x_hbm, x_flat, meta, a_col, q_col, acc, row_acc, s_buf, w_buf, diag,
                  local_sem, first_sem, send_sem, recv_sem, msend_sem, mrecv_sem, out_sem):
    n, d = x_hbm.shape
    chunk = n // CHUNKS
    me = lax.axis_index('seg')
    core = lax.rem(me, 2)
    mate = me + 1 - 2 * core
    right = lax.rem(me + 2, seg_len)
    left = lax.rem(me + seg_len - 2, seg_len)
    right_x = right + 1 - 2 * core
    left_x = left + 1 - 2 * core
    far_x = lax.rem(me + 4, seg_len) + 1 - 2 * core
    scale = math.log2(math.e) * 0.5 / d
    inv_lsq = 1.0 / d

    load = pltpu.make_async_copy(x_hbm, x_flat.at[pl.ds(0, n)], local_sem)
    load.start()

    barrier = pltpu.get_barrier_semaphore()
    for hop in range(1, seg_len):
        pl.semaphore_signal(barrier, inc=1, device_id={'seg': lax.rem(me + hop, seg_len)}, device_id_type=MESH)
    pl.semaphore_wait(barrier, seg_len - 1)

    landing = {1: left_hbm, 2: right_hbm, 3: left_x_hbm, 4: right_x_hbm, 6: x_flat.at[pl.ds(n, n)]}

    def send(kind, k, src, slot, dev):
        rows = pl.ds(pl.multiple_of(k * chunk, chunk), chunk)
        return pltpu.make_async_remote_copy(
            src_ref=src.at[rows], dst_ref=landing[slot].at[rows], send_sem=send_sem.at[kind, k],
            recv_sem=recv_sem.at[slot, k], device_id={'seg': dev}, device_id_type=MESH)

    def to_right(k):
        return send(0, k, x_hbm, 1, right)

    def to_left(k):
        return send(1, k, x_hbm, 2, left)

    def to_mate(k):
        return send(2, k, x_hbm, 6, mate)

    def pass_left_block(k):
        return send(3, k, left_hbm, 3, mate)

    def pass_right_block(k):
        return send(4, k, right_hbm, 4, mate)

    to_right(0).start()
    to_left(0).start()
    load.wait()

    def prologue(r, _):
        rows = pl.ds(pl.multiple_of(r * LANES, LANES), LANES)
        x = x_flat[rows, :].astype(jnp.float32)
        neg = jnp.sum(x * x, axis=1, keepdims=True) * (-scale)
        neg = jnp.broadcast_to(neg, (LANES, LANES))
        a_col[rows, :] = neg
        q_row = q_ref[:, rows]
        meta[0, 1:2, rows] = neg.T[0:1, :]
        meta[0, 0:1, rows] = q_row
        q_col[rows, :] = jnp.broadcast_to(q_row, (LANES, LANES)).T
        row_acc[rows, :] = jnp.zeros((LANES, LANES), jnp.float32)
        acc[rows, :] = jnp.zeros((LANES, d), jnp.float32)
        return 0

    lax.fori_loop(0, n // LANES, prologue, 0)

    to_mate(0).start()
    peers = ((1, right), (2, left), (3, right_x), (4, left_x), (5, far_x), (6, mate))
    metas = [
        pltpu.make_async_remote_copy(
            src_ref=meta.at[0], dst_ref=meta.at[slot], send_sem=msend_sem.at[slot], recv_sem=mrecv_sem.at[slot],
            device_id={'seg': dev}, device_id_type=MESH)
        for slot, dev in peers]
    for copy in metas:
        copy.start()
    columns = {1: reach - 2, 2: reach + 2, 3: reach - 1 - 2 * core, 4: reach + 3 - 2 * core, 5: 2 * reach * core,
               6: reach + 1 - 2 * core}

    def start_rest(k, _):
        to_right(k).start()
        to_left(k).start()
        to_mate(k).start()
        return 0

    lax.fori_loop(1, CHUNKS, start_rest, 0)

    meta[7] = jnp.zeros((2, n), jnp.float32)
    row_id = lax.broadcasted_iota(jnp.int32, (TILE, 2 * TILE), 0)
    col_id = lax.broadcasted_iota(jnp.int32, (TILE, 2 * TILE), 1)
    for half in range(2):
        diag[half] = jnp.where(row_id + half * TILE == col_id, -1e30, 0.0)
    diag[2] = jnp.zeros((TILE, 2 * TILE), jnp.float32)

    def serve(k):
        to_right(k).wait_recv()
        to_left(k).wait_recv()
        pass_left_block(k).start()
        pass_right_block(k).start()

    tiles = n // TILE
    ring = 2 * CHUNKS
    last = ring + 4

    def place(task):
        slot = jnp.where(task < CHUNKS, 0, jnp.where(task < ring, 6, 1 + task - ring))
        k = jnp.where(task < CHUNKS, CHUNKS - 1 - task, jnp.where(task < ring, task - CHUNKS, 0))
        return slot, k

    def block(task):
        slot, k = place(task)
        row = jnp.where(task < ring, jnp.where(slot == 0, 0, n) + k * chunk, 2 * n + (task - ring) * chunk)
        return x_flat[pl.ds(pl.multiple_of(row, chunk), chunk), :]

    def dots(i, task):
        return lax.dot_general(x_flat[i * TILE:(i + 1) * TILE, :], block(task), (((1,), (1,)), ((), ())),
                               preferred_element_type=jnp.float32)

    def weigh(dot_tile, i, slot, k, buf, cap):
        for p in range(TILE // PIECE):
            rows = slice(i * TILE + p * PIECE, i * TILE + (p + 1) * PIECE)
            tile_rows = slice(p * PIECE, (p + 1) * PIECE)
            a_piece = a_col[rows, :]
            q_piece = q_col[rows, :]
            part = row_acc[rows, :]
            for h in range(chunk // LANES):
                lanes = slice(h * LANES, (h + 1) * LANES)
                cols = pl.ds(pl.multiple_of(k * chunk + h * LANES, LANES), LANES)
                power = (dot_tile[tile_rows, lanes] * (2.0 * scale) + a_piece) + meta[slot, 1:2, cols]
                power = jnp.minimum(power, 0.0 if cap is None else diag[cap, tile_rows, lanes])
                w = jnp.exp2(power) * meta[slot, 0:1, cols] * q_piece
                part = part + w
                w_buf[buf, tile_rows, lanes] = w.astype(jnp.bfloat16)
            row_acc[rows, :] = part

    def pull(i, task, buf):
        acc[i * TILE:(i + 1) * TILE, :] += jnp.dot(w_buf[buf], block(task), preferred_element_type=jnp.float32)

    def run_task(task, own):
        slot, k = place(task)
        was = jnp.maximum(task - 1, 0)
        was_slot, was_k = place(was)
        was_meta = jnp.where(task == 0, 7, was_slot)
        held = s_buf[...]
        for i in range(tiles):
            i1, task1, k1, meta1 = (tiles - 1, was, was_k, was_meta) if i == 0 else (i - 1, task, k, slot)
            cap = None
            if own:
                step = i1 - 2 * k1
                cap = jnp.where((step == 0) | (step == 1), step, 2)
            fresh = dots(i, task)
            weigh(held, i1, meta1, k1, i % 2, cap)
            pull(i1, task1, i % 2)
            held = fresh
        s_buf[...] = held

    s_buf[...] = jnp.zeros(s_buf.shape, jnp.float32)

    def own_task(task, _):
        @pl.when(task == CHUNKS - 1)
        def _():
            for copy in metas:
                copy.wait_recv()
            for s, column in columns.items():
                meta[s, 0:1, :] = jnp.where(band_ref[0, column] != 0, meta[s, 0:1, :], 0.0)

            def wait_mate(k, _):
                to_mate(k).wait_recv()
                return 0

            lax.fori_loop(0, CHUNKS, wait_mate, 0)
            serve(0)

        run_task(task, True)
        return 0

    lax.fori_loop(0, CHUNKS, own_task, 0)

    firsts = [
        pltpu.make_async_copy(landing[slot].at[pl.ds(0, chunk)],
                              x_flat.at[pl.ds(2 * n + (slot - 1) * chunk, chunk)], first_sem.at[slot])
        for slot in range(1, 5)]

    def other_task(task, _):
        @pl.when(task == ring - 2)
        def _():
            pass_left_block(0).wait_recv()
            pass_right_block(0).wait_recv()
            for copy in firsts:
                copy.start()

        @pl.when(task == ring - 1)
        def _():
            for copy in firsts:
                copy.wait()

        for k in range(1, CHUNKS - 1):
            @pl.when(task == SERVE[k])
            def _(k=k):
                serve(k)

        run_task(task, False)
        return 0

    lax.fori_loop(CHUNKS, last, other_task, 0)

    slot, k = place(last - 1)
    weigh(s_buf[...], tiles - 1, slot, k, 0, None)
    pull(tiles - 1, last - 1, 0)

    outs = [pltpu.make_async_copy(src, dst, out_sem.at[j])
            for j, (src, dst) in enumerate(((acc, acc_hbm), (row_acc, row_hbm), (a_col, a_hbm), (q_col, q_hbm), (meta, meta_hbm)))]
    for copy in outs:
        copy.start()
    serve(CHUNKS - 1)

    def drain(k, _):
        for copy in (to_right, to_left, to_mate, pass_left_block, pass_right_block):
            copy(k).wait_send()
        return 0

    def arrive(k, _):
        pass_left_block(k).wait_recv()
        pass_right_block(k).wait_recv()
        return 0

    lax.fori_loop(0, CHUNKS, drain, 0)
    lax.fori_loop(1, CHUNKS, arrive, 0)
    for copy in metas:
        copy.wait_send()
    for copy in outs:
        copy.wait()


def pair_kernel(parts, final, meta_rows, band_ref, x_hbm, a_hbm, q_hbm, *refs):
    n, d = x_hbm.shape
    n_src = len(parts)
    sources, refs = refs[:n_src], refs[n_src:]
    meta_hbm, refs = refs[0], refs[1:]
    if final:
        acc_old, row_old, acc_new, row_new, f_hbm, e_ref = refs[:6]
        (x_own, vis, meta, meta_all, a_col, q_col, acc, row_acc, w_buf, acc_in, row_in, load_sem, vis_sem, old_sem,
         out_sem) = refs[6:]
    else:
        acc_hbm, row_hbm = refs[:2]
        x_own, vis, meta, meta_all, a_col, q_col, acc, row_acc, w_buf, load_sem, vis_sem, out_sem = refs[2:]
    chunk = n // CHUNKS
    tasks = sum(count for _, _, count, _, _ in parts)
    tiles = n // TILE
    core = lax.rem(lax.axis_index('seg'), 2)
    scale = math.log2(math.e) * 0.5 / d

    def fetch(source, k, task):
        return pltpu.make_async_copy(source.at[pl.ds(k * chunk, chunk)], vis.at[pl.ds(task * chunk, chunk)],
                                     vis_sem.at[task])

    plan = []
    for source, (want, first, count, slot, column) in zip(sources, parts):
        plan += [(source, want, first + j, slot, column) for j in range(count)]
    plan_tasks = meta_rows(plan)

    def start_fetch(task):
        for source, want, k in plan_tasks[task][0]:
            if want is None:
                fetch(source, k, task).start()
            else:
                @pl.when(core == want)
                def _():
                    fetch(source, k, task).start()

    loads = [pltpu.make_async_copy(src, dst, load_sem.at[j])
             for j, (src, dst) in enumerate(((meta_hbm, meta_all), (x_hbm, x_own), (a_hbm, a_col), (q_hbm, q_col)))]
    n_tasks = len(plan_tasks)
    start_fetch(0)
    for copy in loads:
        copy.start()
    for task in range(1, n_tasks):
        start_fetch(task)
    if final:
        olds = [pltpu.make_async_copy(src, dst, old_sem.at[j])
                for j, (src, dst) in enumerate(((acc_old, acc_in.at[0]), (acc_new, acc_in.at[1]),
                                                (row_old, row_in.at[0]), (row_new, row_in.at[1])))]
        for copy in olds:
            copy.start()

    def clear(r, _):
        rows = pl.ds(pl.multiple_of(r * LANES, LANES), LANES)
        acc[rows, :] = jnp.zeros((LANES, d), jnp.float32)
        row_acc[rows, :] = jnp.zeros((LANES, LANES), jnp.float32)
        return 0

    lax.fori_loop(0, n // LANES, clear, 0)
    w_buf[...] = jnp.zeros(w_buf.shape, jnp.bfloat16)
    for copy in loads:
        copy.wait()
    for task in range(n_tasks):
        _, k, slot, column = plan_tasks[task]
        cols = slice(task * chunk, (task + 1) * chunk)
        own_cols = slice(k * chunk, (k + 1) * chunk)
        meta[0:1, cols] = jnp.where(band_ref[0, column(core)] != 0, meta_all[slot, 0:1, own_cols], 0.0)
        meta[1:2, cols] = meta_all[slot, 1:2, own_cols]
    meta[:, n_tasks * chunk:(n_tasks + 1) * chunk] = jnp.zeros((2, chunk), jnp.float32)

    def arrived(task):
        fetch(sources[0], 0, task).wait()

    def product(acc1, acc2):
        def push(task, rows_half, cols_half, register, mxu, transpose):
            rows = pl.ds(pl.multiple_of(task * chunk + rows_half * TILE, TILE), TILE)
            tile = vis[rows, cols_half * TILE:(cols_half + 1) * TILE]
            pltpu.matmul_push_rhs(tile, register, mxu, transpose=transpose)

        def push_dots(task, half):
            for mxu in range(2):
                push(task, mxu, half, half, mxu, True)

        def push_pull(task, half):
            for mxu in range(2):
                push(task, half, mxu, half, mxu, False)

        def piece_rows(i, p):
            return pl.ds(pl.multiple_of(i * TILE + p * PIECE, PIECE), PIECE)

        def dots(i, buf, half):
            for p in range(PIECES):
                lhs = x_own[piece_rows(i, p), half * TILE:(half + 1) * TILE]
                for mxu in range(2):
                    pltpu.matmul_acc_lhs(acc1[buf][mxu][p], lhs, load_staged_rhs=half if p == 0 else None)

        def pull(buf, half):
            for p in range(PIECES):
                lhs = w_buf[buf, p * PIECE:(p + 1) * PIECE, half * TILE:(half + 1) * TILE]
                for mxu in range(2):
                    pltpu.matmul_acc_lhs(acc2[mxu][p], lhs, load_staged_rhs=half if p == 0 else None)

        def weigh(i, task, buf, mxu):
            for p in range(PIECES):
                rows = piece_rows(i, p)
                dot_piece = pltpu.matmul_pop(acc1[buf][mxu][p])
                a_piece = a_col[rows, :]
                q_piece = q_col[rows, :]
                part = row_acc[rows, :]
                for h in range(TILE // LANES):
                    first = mxu * TILE + h * LANES
                    cols = pl.ds(pl.multiple_of(task * chunk + first, LANES), LANES)
                    power = (dot_piece[:, h * LANES:(h + 1) * LANES] * (2.0 * scale) + a_piece) + meta[1:2, cols]
                    power = jnp.minimum(power, 0.0)
                    w = jnp.exp2(power) * meta[0:1, cols] * q_piece
                    part = part + w
                    w_buf[buf, p * PIECE:(p + 1) * PIECE, first:first + LANES] = w.astype(jnp.bfloat16)
                row_acc[rows, :] = part

        def take_pull(i):
            for p in range(PIECES):
                rows = piece_rows(i, p)
                for mxu in range(2):
                    acc[rows, mxu * TILE:(mxu + 1) * TILE] += pltpu.matmul_pop(acc2[mxu][p])

        def run_task(task, _):
            was = jnp.maximum(task - 1, 0)
            was_meta = jnp.where(task == 0, n_tasks, was)
            coming = jnp.minimum(task + 1, n_tasks - 1)

            @pl.when(task + 1 < n_tasks)
            def _():
                arrived(task + 1)

            def body(g, _):
                for u in range(UNROLL):
                    i = g * UNROLL + u
                    buf = u % 2
                    task1, meta1, task3 = task, task, task
                    if u == 0:
                        i1, i2 = lax.rem(i + tiles - 1, tiles), lax.rem(i + tiles - 2, tiles)
                        task1, meta1 = jnp.where(g == 0, was, task), jnp.where(g == 0, was_meta, task)
                    else:
                        i1 = i - 1
                        i2 = lax.rem(i + tiles - 2, tiles) if u == 1 else i - 2
                    if u == UNROLL - 1:
                        task3 = jnp.where(g == tiles // UNROLL - 1, coming, task)
                    dots(i, buf, 0)
                    push_pull(task1, 0)
                    weigh(i1, meta1, 1 - buf, 0)
                    dots(i, buf, 1)
                    push_pull(task1, 1)
                    take_pull(i2)
                    weigh(i1, meta1, 1 - buf, 1)
                    pull(1 - buf, 0)
                    push_dots(task3, 0)
                    pull(1 - buf, 1)
                    push_dots(task3, 1)
                return 0

            lax.fori_loop(0, tiles // UNROLL, body, 0)
            return 0

        for refs in acc1[0] + acc1[1] + acc2:
            for ref in refs:
                pltpu.matmul_pop(ref)
        arrived(0)
        push_dots(0, 0)
        push_dots(0, 1)
        lax.fori_loop(0, n_tasks, run_task, 0)

        spare = x_own[0:PIECE, 0:TILE]
        for half in range(2):
            for mxu in range(2):
                pltpu.matmul_acc_lhs(acc1[0][mxu][0], spare, load_staged_rhs=half)
            push_pull(n_tasks - 1, half)
        for mxu in range(2):
            pltpu.matmul_pop(acc1[0][mxu][0])
        take_pull(tiles - 2)
        weigh(tiles - 1, n_tasks - 1, 1, 0)
        weigh(tiles - 1, n_tasks - 1, 1, 1)
        pull(1, 0)
        pull(1, 1)
        take_pull(tiles - 1)

    piece = [[pltpu.ACC(mxu)((PIECE, TILE), jnp.float32) for _ in range(PIECES)] for mxu in range(2)]
    pl.run_scoped(product, (piece, piece), piece)

    if not final:
        outs = [pltpu.make_async_copy(src, dst, out_sem.at[j])
                for j, (src, dst) in enumerate(((acc, acc_hbm), (row_acc, row_hbm)))]
        for copy in outs:
            copy.start()
        for copy in outs:
            copy.wait()
        return

    for copy in olds:
        copy.wait()

    def out_copy(r):
        rows = pl.ds(pl.multiple_of(r * LANES, LANES), LANES)
        return pltpu.make_async_copy(acc.at[rows], f_hbm.at[rows], out_sem.at[r])

    def finish(r, total):
        rows = pl.ds(pl.multiple_of(r * LANES, LANES), LANES)
        row_parts = row_acc[rows, :] + (row_in[0, rows, :] + row_in[1, rows, :])
        row_sum = jnp.sum(row_parts, axis=1, keepdims=True)
        pulls = acc[rows, :] + (acc_in[0, rows, :] + acc_in[1, rows, :])
        acc[rows, :] = (row_sum * x_own[rows, :].astype(jnp.float32) - pulls) * (1.0 / d)
        out_copy(r).start()
        return total + jnp.sum(row_parts.reshape(LANES // 8, 8, LANES), axis=0)

    total = lax.fori_loop(0, n // LANES, finish, jnp.zeros((8, LANES), jnp.float32))
    e_ref[...] = jnp.broadcast_to(0.5 * jnp.sum(total), (8, LANES))

    def drain_out(r, _):
        out_copy(r).wait()
        return 0

    lax.fori_loop(0, n // LANES, drain_out, 0)


def by_task(plan):
    tasks, twins = [], {}
    for source, want, k, slot, column in plan:
        if want is not None and (slot, k) in twins:
            tasks[twins[slot, k]][0].append((source, want, k))
            continue
        twins[slot, k] = len(tasks)
        tasks.append(([(source, want, k)], k, slot, column))
    return tasks


def energy_kernel(seg_len, e_in, e_ref, e_buf, esend_sem, erecv_sem):
    me = lax.axis_index('seg')
    e_buf[me] = e_in[...]
    barrier = pltpu.get_barrier_semaphore()
    for hop in range(1, seg_len):
        pl.semaphore_signal(barrier, inc=1, device_id={'seg': lax.rem(me + hop, seg_len)}, device_id_type=MESH)
    pl.semaphore_wait(barrier, seg_len - 1)
    energy = [
        pltpu.make_async_remote_copy(
            src_ref=e_in, dst_ref=e_buf.at[me], send_sem=esend_sem.at[hop], recv_sem=erecv_sem.at[hop],
            device_id={'seg': lax.rem(me + hop, seg_len)}, device_id_type=MESH)
        for hop in range(1, seg_len)]
    for copy in energy:
        copy.start()
    for copy in energy:
        copy.wait()
    e_sum = e_buf[0]
    for dev in range(1, seg_len):
        e_sum = e_sum + e_buf[dev]
    e_ref[...] = e_sum


def solution(mesh):
    seg_len = mesh.shape['seg']

    def device_fn(positions, charges, pair_band):
        n, d = positions.shape
        reach = (pair_band.shape[1] - 1) // 2
        chunk = n // CHUNKS
        hbm, vmem, smem = (pl.BlockSpec(memory_space=m) for m in (pl.ANY, pltpu.VMEM, pltpu.SMEM))
        f32, bf16, dma = jnp.float32, jnp.bfloat16, pltpu.SemaphoreType.DMA
        sums = (jax.ShapeDtypeStruct((n, d), f32), jax.ShapeDtypeStruct((n, LANES), f32))
        cols = (jax.ShapeDtypeStruct((n, LANES), f32),) * 2
        block = jax.ShapeDtypeStruct((n, d), bf16)

        def cost(chunks):
            return pl.CostEstimate(flops=4 * n * chunk * d * chunks, bytes_accessed=16 * n * d, transcendentals=0)

        acc_a, row_a, a_col, q_col, meta, left, right, left_x, right_x = pl.pallas_call(
            functools.partial(gather_kernel, seg_len, reach),
            out_shape=sums + cols + (jax.ShapeDtypeStruct((8, 2, n), f32),) + (block,) * 4,
            in_specs=[smem, hbm, vmem],
            out_specs=(hbm,) * 9,
            scratch_shapes=[
                pltpu.VMEM((2 * n + 4 * chunk, d), bf16),
                pltpu.VMEM((8, 2, n), f32),
                pltpu.VMEM((n, LANES), f32),
                pltpu.VMEM((n, LANES), f32),
                pltpu.VMEM((n, d), f32),
                pltpu.VMEM((n, LANES), f32),
                pltpu.VMEM((TILE, chunk), f32),
                pltpu.VMEM((2, TILE, chunk), bf16),
                pltpu.VMEM((3, TILE, chunk), f32),
                dma, dma((5,)), dma((5, CHUNKS)), dma((7, CHUNKS)), dma((7,)), dma((7,)), dma((5,)),
            ],
            compiler_params=pltpu.CompilerParams(
                collective_id=0, has_side_effects=True, vmem_limit_bytes=60 * 2**20),
            cost_estimate=cost(2 * CHUNKS + 4),
            name='gather_pairs',
        )(pair_band, positions, charges.reshape(1, n))

        ups = [(dev, (dev + 1) % seg_len) for dev in range(1, seg_len, 2)]
        downs = [(dev, (dev - 1) % seg_len) for dev in range(0, seg_len, 2)]
        far_up = lax.ppermute(left, 'seg', ups)
        far_down = lax.ppermute(right, 'seg', downs)

        def pairs(parts, sources, old):
            final = old is not None
            count = len({(slot, first + j) for want, first, number, slot, _ in parts for j in range(number)})
            scratch = [
                pltpu.VMEM((n, d), bf16), pltpu.VMEM((count * chunk, d), bf16), pltpu.VMEM((2, (count + 1) * chunk), f32),
                pltpu.VMEM((8, 2, n), f32), pltpu.VMEM((n, LANES), f32), pltpu.VMEM((n, LANES), f32), pltpu.VMEM((n, d), f32),
                pltpu.VMEM((n, LANES), f32), pltpu.VMEM((2, TILE, chunk), bf16)]
            if final:
                scratch += [pltpu.VMEM((2, n, d), f32), pltpu.VMEM((2, n, LANES), f32)]
            scratch += [dma((4,)), dma((count,))] + ([dma((4,)), dma((n // LANES,))] if final else [dma((2,))])
            old = old or ()
            return pl.pallas_call(
                functools.partial(pair_kernel, parts, final, by_task),
                out_shape=(sums[0], jax.ShapeDtypeStruct((8, LANES), f32)) if final else sums,
                in_specs=[smem] + [hbm] * (4 + len(sources) + len(old)),
                out_specs=(hbm, vmem) if final else (hbm, hbm),
                scratch_shapes=scratch,
                compiler_params=pltpu.CompilerParams(vmem_limit_bytes=60 * 2**20),
                cost_estimate=cost(count),
                name='far_pairs' if final else 'ring_pairs',
            )(pair_band, positions, a_col, q_col, *sources, meta, *old)

        rest = CHUNKS - 1
        ring_parts = (
            (None, 1, rest, 1, lambda core: reach - 2), (None, 1, rest, 2, lambda core: reach + 2),
            (None, 1, rest, 3, lambda core: reach - 1 - 2 * core), (None, 1, rest, 4, lambda core: reach + 3 - 2 * core))
        acc_b, row_b = pairs(ring_parts, (left, right, left_x, right_x), None)
        far_parts = ((0, 0, CHUNKS, 5, lambda core: 2 * reach * core), (1, 0, CHUNKS, 5, lambda core: 2 * reach * core))
        forces, share = pairs(far_parts, (far_up, far_down), (acc_a, row_a, acc_b, row_b))
        energy = pl.pallas_call(
            functools.partial(energy_kernel, seg_len),
            out_shape=jax.ShapeDtypeStruct((8, LANES), f32),
            in_specs=[vmem],
            out_specs=vmem,
            scratch_shapes=[pltpu.VMEM((seg_len, 8, LANES), f32), dma((seg_len,)), dma((seg_len,))],
            compiler_params=pltpu.CompilerParams(collective_id=1, has_side_effects=True),
            name='energy',
        )(share)
        return forces, energy[0, 0].reshape(1)

    row_spec = P(('sys', 'seg'), None)
    vec_spec = P(('sys', 'seg'))
    return jax.shard_map(device_fn, mesh=mesh, in_specs=(row_spec, vec_spec, row_spec), out_specs=(row_spec, P('sys')), check_vma=False)
```

```python
import functools
import math

import jax
import jax.numpy as jnp
from jax import lax
from jax.experimental import pallas as pl
from jax.experimental.pallas import tpu as pltpu
from jax.sharding import PartitionSpec as P

MESH = pl.DeviceIdType.MESH
LANES = 128
CHUNKS = 6
TILE = 256
PIECE = 128


def kernel(seg_len, reach, band_ref, x_hbm, q_ref, f_hbm, e_ref, x_all, meta, a_col, q_col, acc, row_acc, s_buf, w_buf, diag, e_buf,
           local_sem, send_sem, recv_sem, msend_sem, mrecv_sem, esend_sem, erecv_sem, out_sem):
    n, d = x_hbm.shape
    chunk = n // CHUNKS
    me = lax.axis_index('seg')
    core = lax.rem(me, 2)
    mate = me + 1 - 2 * core
    right = lax.rem(me + 2, seg_len)
    left = lax.rem(me + seg_len - 2, seg_len)
    right_x = right + 1 - 2 * core
    left_x = left + 1 - 2 * core
    far_x = lax.rem(me + 4, seg_len) + 1 - 2 * core
    scale = math.log2(math.e) * 0.5 / d
    inv_lsq = 1.0 / d

    load = pltpu.make_async_copy(x_hbm, x_all.at[0], local_sem)
    load.start()

    barrier = pltpu.get_barrier_semaphore()
    for hop in range(1, seg_len):
        pl.semaphore_signal(barrier, inc=1, device_id={'seg': lax.rem(me + hop, seg_len)}, device_id_type=MESH)

    def send(kind, k, src, slot, dev):
        rows = pl.ds(pl.multiple_of(k * chunk, chunk), chunk)
        return pltpu.make_async_remote_copy(
            src_ref=src.at[rows], dst_ref=x_all.at[slot, rows], send_sem=send_sem.at[kind, k],
            recv_sem=recv_sem.at[slot, k], device_id={'seg': dev}, device_id_type=MESH)

    def to_right(k):
        return send(0, k, x_hbm, 1, right)

    def to_left(k):
        return send(1, k, x_hbm, 2, left)

    def to_mate(k):
        return send(2, k, x_hbm, 6, mate)

    def pass_left_block(k):
        return send(3, k, x_all.at[1], 3, mate)

    def pass_right_block(k):
        return send(4, k, x_all.at[2], 4, mate)

    def pass_far(k):
        onward = core * right_x + (1 - core) * left_x
        return send(5, k, x_all.at[2 - core], 5, onward)

    load.wait()

    def prologue(r):
        rows = pl.ds(pl.multiple_of(r * LANES, LANES), LANES)
        x = x_all[0, rows, :].astype(jnp.float32)
        neg = jnp.sum(x * x, axis=1, keepdims=True) * (-scale)
        neg = jnp.broadcast_to(neg, (LANES, LANES))
        a_col[rows, :] = neg
        q_row = q_ref[:, rows]
        meta[0, 1:2, rows] = neg.T[0:1, :]
        meta[0, 0:1, rows] = q_row
        q_col[rows, :] = jnp.broadcast_to(q_row, (LANES, LANES)).T
        row_acc[rows, :] = jnp.zeros((LANES, LANES), jnp.float32)
        acc[rows, :] = jnp.zeros((LANES, d), jnp.float32)

    def prologues(r, _):
        for u in range(chunk // LANES):
            prologue(r * (chunk // LANES) + u)
        return 0

    lax.fori_loop(0, CHUNKS, prologues, 0)
    pl.semaphore_wait(barrier, seg_len - 1)

    for copy in (to_mate, to_right, to_left):
        copy(0).start()
    peers = ((1, right), (2, left), (3, right_x), (4, left_x), (5, far_x), (6, mate))
    metas = [
        pltpu.make_async_remote_copy(
            src_ref=meta.at[0], dst_ref=meta.at[slot], send_sem=msend_sem.at[slot], recv_sem=mrecv_sem.at[slot],
            device_id={'seg': dev}, device_id_type=MESH)
        for slot, dev in peers]
    for copy in metas:
        copy.start()
    columns = {1: reach - 2, 2: reach + 2, 3: reach - 1 - 2 * core, 4: reach + 3 - 2 * core, 5: 2 * reach * core,
               6: reach + 1 - 2 * core}

    def start_rest(k, _):
        to_right(k).start()
        to_left(k).start()
        to_mate(k).start()
        return 0

    lax.fori_loop(1, CHUNKS, start_rest, 0)

    meta[7] = jnp.zeros((2, n), jnp.float32)
    row_id = lax.broadcasted_iota(jnp.int32, (TILE, 2 * TILE), 0)
    col_id = lax.broadcasted_iota(jnp.int32, (TILE, 2 * TILE), 1)
    for half in range(2):
        diag[half] = jnp.where(row_id + half * TILE == col_id, -1e30, 0.0)
    diag[2] = jnp.zeros((TILE, 2 * TILE), jnp.float32)

    def serve(k):
        to_right(k).wait_recv()
        to_left(k).wait_recv()
        pass_left_block(k).start()
        pass_right_block(k).start()
        pass_far(k).start()

    tiles = n // TILE
    ring = 2 * CHUNKS
    last = ring + 4 * CHUNKS

    def place(task):
        turn = task - ring
        slot = jnp.where(task < CHUNKS, 0, jnp.where(task < ring, 6, jnp.where(task < last, 1 + lax.rem(turn, 4), 5)))
        k = jnp.where(task < CHUNKS, CHUNKS - 1 - task,
                      jnp.where(task < ring, task - CHUNKS, jnp.where(task < last, turn // 4, task - last)))
        return slot, k

    def block(slot, k):
        return x_all[slot, pl.ds(pl.multiple_of(k * chunk, chunk), chunk), :]

    def dots(i, slot, k):
        return lax.dot_general(x_all[0, i * TILE:(i + 1) * TILE, :], block(slot, k), (((1,), (1,)), ((), ())),
                               preferred_element_type=jnp.float32)

    def weigh(dot_tile, i, slot, k, buf, cap):
        for p in range(TILE // PIECE):
            rows = slice(i * TILE + p * PIECE, i * TILE + (p + 1) * PIECE)
            tile_rows = slice(p * PIECE, (p + 1) * PIECE)
            a_piece = a_col[rows, :]
            q_piece = q_col[rows, :]
            part = row_acc[rows, :]
            for h in range(chunk // LANES):
                lanes = slice(h * LANES, (h + 1) * LANES)
                cols = pl.ds(pl.multiple_of(k * chunk + h * LANES, LANES), LANES)
                power = (dot_tile[tile_rows, lanes] * (2.0 * scale) + a_piece) + meta[slot, 1:2, cols]
                power = jnp.minimum(power, 0.0 if cap is None else diag[cap, tile_rows, lanes])
                w = jnp.exp2(power) * meta[slot, 0:1, cols] * q_piece
                part = part + w
                w_buf[buf, tile_rows, lanes] = w.astype(jnp.bfloat16)
            row_acc[rows, :] = part

    def pull(i, slot, k, buf):
        acc[i * TILE:(i + 1) * TILE, :] += jnp.dot(w_buf[buf], block(slot, k), preferred_element_type=jnp.float32)

    def run_task(task, own):
        slot, k = place(task)
        was_slot, was_k = place(jnp.maximum(task - 1, 0))
        was_meta = jnp.where(task == 0, 7, was_slot)
        held = s_buf[...]
        for i in range(tiles):
            i1, slot1, k1, meta1 = (tiles - 1, was_slot, was_k, was_meta) if i == 0 else (i - 1, slot, k, slot)
            cap = None
            if own:
                step = i1 - 2 * k1
                cap = jnp.where((step == 0) | (step == 1), step, 2)
            fresh = dots(i, slot, k)
            weigh(held, i1, meta1, k1, i % 2, cap)
            pull(i1, slot1, k1, i % 2)
            held = fresh
        s_buf[...] = held

    s_buf[...] = jnp.zeros(s_buf.shape, jnp.float32)

    def own_task(task, _):
        @pl.when(task == CHUNKS - 1)
        def _():
            for copy in metas:
                copy.wait_recv()
            for s, column in columns.items():
                meta[s, 0:1, :] = jnp.where(band_ref[0, column] != 0, meta[s, 0:1, :], 0.0)

            def wait_mate(k, _):
                to_mate(k).wait_recv()
                return 0

            lax.fori_loop(0, CHUNKS, wait_mate, 0)
            serve(0)

        run_task(task, True)
        return 0

    lax.fori_loop(0, CHUNKS, own_task, 0)

    def other_task(task, _):
        coming = task + 1 - ring
        k = coming // 4

        @pl.when((coming >= 0) & (lax.rem(coming, 4) == 0) & (k < CHUNKS))
        def _():
            pass_left_block(k).wait_recv()
            pass_right_block(k).wait_recv()

            @pl.when(k + 1 < CHUNKS)
            def _():
                serve(k + 1)

        @pl.when((task + 1 >= last) & (task + 1 < last + CHUNKS))
        def _():
            pass_far(task + 1 - last).wait_recv()

        run_task(task, False)
        return 0

    lax.fori_loop(CHUNKS, last + CHUNKS, other_task, 0)

    slot, k = place(last + CHUNKS - 1)
    weigh(s_buf[...], tiles - 1, slot, k, 0, None)
    pull(tiles - 1, slot, k, 0)

    total = jnp.zeros((8, LANES), jnp.float32)

    def add_rows(r, total):
        rows = pl.ds(pl.multiple_of(r * LANES, LANES), LANES)
        return total + jnp.sum(row_acc[rows, :].reshape(LANES // 8, 8, LANES), axis=0)

    total = lax.fori_loop(0, n // LANES, add_rows, total)
    e_buf[me] = jnp.broadcast_to(0.5 * jnp.sum(total), (8, LANES))

    def finish(r, _):
        rows = pl.ds(pl.multiple_of(r * LANES, LANES), LANES)
        row_sum = jnp.sum(row_acc[rows, :], axis=1, keepdims=True)
        acc[rows, :] = (row_sum * x_all[0, rows, :].astype(jnp.float32) - acc[rows, :]) * inv_lsq
        return 0

    def out_copy(r):
        rows = pl.ds(pl.multiple_of(r * LANES, LANES), LANES)
        return pltpu.make_async_copy(acc.at[rows], f_hbm.at[rows], out_sem.at[r])

    finish(0, 0)
    energy = [
        pltpu.make_async_remote_copy(
            src_ref=e_buf.at[me], dst_ref=e_buf.at[me], send_sem=esend_sem.at[hop], recv_sem=erecv_sem.at[hop],
            device_id={'seg': lax.rem(me + hop, seg_len)}, device_id_type=MESH)
        for hop in range(1, seg_len)]
    for copy in energy:
        copy.start()

    def finish_and_send(r, _):
        finish(r, 0)
        out_copy(r - 1).start()
        return 0

    lax.fori_loop(1, n // LANES, finish_and_send, 0)
    out_copy(n // LANES - 1).start()

    def drain(k, _):
        for copy in (to_right, to_left, to_mate, pass_left_block, pass_right_block, pass_far):
            copy(k).wait_send()
        return 0

    lax.fori_loop(0, CHUNKS, drain, 0)
    for copy in metas:
        copy.wait_send()
    for copy in energy:
        copy.wait()
    e_sum = e_buf[0]
    for dev in range(1, seg_len):
        e_sum = e_sum + e_buf[dev]
    e_ref[0, 0] = e_sum[0, 0]

    def drain_out(r, _):
        out_copy(r).wait()
        return 0

    lax.fori_loop(0, n // LANES, drain_out, 0)


def solution(mesh):
    seg_len = mesh.shape['seg']

    def device_fn(positions, charges, pair_band):
        n, d = positions.shape
        reach = (pair_band.shape[1] - 1) // 2
        flops = 4 * n * n * d * (2 * reach + 1)
        forces, energy = pl.pallas_call(
            functools.partial(kernel, seg_len, reach),
            out_shape=(jax.ShapeDtypeStruct((n, d), jnp.float32), jax.ShapeDtypeStruct((1, 1), jnp.float32)),
            in_specs=[pl.BlockSpec(memory_space=pltpu.SMEM), pl.BlockSpec(memory_space=pl.ANY),
                      pl.BlockSpec(memory_space=pltpu.VMEM)],
            out_specs=(pl.BlockSpec(memory_space=pl.ANY), pl.BlockSpec(memory_space=pltpu.SMEM)),
            scratch_shapes=[
                pltpu.VMEM((7, n, d), jnp.bfloat16),
                pltpu.VMEM((8, 2, n), jnp.float32),
                pltpu.VMEM((n, LANES), jnp.float32),
                pltpu.VMEM((n, LANES), jnp.float32),
                pltpu.VMEM((n, d), jnp.float32),
                pltpu.VMEM((n, LANES), jnp.float32),
                pltpu.VMEM((TILE, 2 * TILE), jnp.float32),
                pltpu.VMEM((2, TILE, 2 * TILE), jnp.bfloat16),
                pltpu.VMEM((3, TILE, 2 * TILE), jnp.float32),
                pltpu.VMEM((seg_len, 8, LANES), jnp.float32),
                pltpu.SemaphoreType.DMA,
                pltpu.SemaphoreType.DMA((6, CHUNKS)),
                pltpu.SemaphoreType.DMA((7, CHUNKS)),
                pltpu.SemaphoreType.DMA((7,)),
                pltpu.SemaphoreType.DMA((7,)),
                pltpu.SemaphoreType.DMA((seg_len,)),
                pltpu.SemaphoreType.DMA((seg_len,)),
                pltpu.SemaphoreType.DMA((n // LANES,)),
            ],
            compiler_params=pltpu.CompilerParams(
                collective_id=0, has_side_effects=True, vmem_limit_bytes=60 * 2**20),
            cost_estimate=pl.CostEstimate(flops=flops, bytes_accessed=16 * n * d, transcendentals=0),
            name='pair_forces',
        )(pair_band, positions, charges.reshape(1, n))
        return forces, energy.reshape(1)

    row_spec = P(('sys', 'seg'), None)
    vec_spec = P(('sys', 'seg'))
    return jax.shard_map(device_fn, mesh=mesh, in_specs=(row_spec, vec_spec, row_spec), out_specs=(row_spec, P('sys')), check_vma=False)
```

```python
import functools
import math

import jax
import jax.numpy as jnp
from jax import lax
from jax.experimental import pallas as pl
from jax.experimental.pallas import tpu as pltpu
from jax.sharding import PartitionSpec as P

MESH = pl.DeviceIdType.MESH
LANES = 128
CHUNKS = 6
TILE = 256
PIECE = 128


def kernel(seg_len, reach, band_ref, x_hbm, q_ref, f_hbm, e_ref, x_all, meta, a_col, q_col, acc, row_acc, s_buf, w_buf, diag, e_buf,
           local_sem, send_sem, recv_sem, msend_sem, mrecv_sem, esend_sem, erecv_sem, out_sem):
    n, d = x_hbm.shape
    chunk = n // CHUNKS
    me = lax.axis_index('seg')
    core = lax.rem(me, 2)
    mate = me + 1 - 2 * core
    right = lax.rem(me + 2, seg_len)
    left = lax.rem(me + seg_len - 2, seg_len)
    right_x = right + 1 - 2 * core
    left_x = left + 1 - 2 * core
    far_x = lax.rem(me + 4, seg_len) + 1 - 2 * core
    scale = math.log2(math.e) * 0.5 / d
    inv_lsq = 1.0 / d

    load = pltpu.make_async_copy(x_hbm, x_all.at[0], local_sem)
    load.start()

    barrier = pltpu.get_barrier_semaphore()
    for hop in range(1, seg_len):
        pl.semaphore_signal(barrier, inc=1, device_id={'seg': lax.rem(me + hop, seg_len)}, device_id_type=MESH)

    def send(kind, k, src, slot, dev):
        rows = pl.ds(pl.multiple_of(k * chunk, chunk), chunk)
        return pltpu.make_async_remote_copy(
            src_ref=src.at[rows], dst_ref=x_all.at[slot, rows], send_sem=send_sem.at[kind, k],
            recv_sem=recv_sem.at[slot, k], device_id={'seg': dev}, device_id_type=MESH)

    def to_right(k):
        return send(0, k, x_hbm, 1, right)

    def to_left(k):
        return send(1, k, x_hbm, 2, left)

    def to_mate(k):
        return send(2, k, x_hbm, 6, mate)

    def pass_left_block(k):
        return send(3, k, x_all.at[1], 3, mate)

    def pass_right_block(k):
        return send(4, k, x_all.at[2], 4, mate)

    def pass_far(k):
        onward = core * right_x + (1 - core) * left_x
        return send(5, k, x_all.at[2 - core], 5, onward)

    load.wait()

    def prologue(r):
        rows = pl.ds(pl.multiple_of(r * LANES, LANES), LANES)
        x = x_all[0, rows, :].astype(jnp.float32)
        neg = jnp.sum(x * x, axis=1, keepdims=True) * (-scale)
        neg = jnp.broadcast_to(neg, (LANES, LANES))
        a_col[rows, :] = neg
        q_row = q_ref[:, rows]
        meta[0, 1:2, rows] = neg.T[0:1, :]
        meta[0, 0:1, rows] = q_row
        q_col[rows, :] = jnp.broadcast_to(q_row, (LANES, LANES)).T
        row_acc[rows, :] = jnp.zeros((LANES, LANES), jnp.float32)
        acc[rows, :] = jnp.zeros((LANES, d), jnp.float32)

    def prologues(r, _):
        for u in range(chunk // LANES):
            prologue(r * (chunk // LANES) + u)
        return 0

    lax.fori_loop(0, CHUNKS, prologues, 0)
    pl.semaphore_wait(barrier, seg_len - 1)

    for copy in (to_mate, to_right, to_left):
        copy(0).start()
    peers = ((1, right), (2, left), (3, right_x), (4, left_x), (5, far_x), (6, mate))
    metas = [
        pltpu.make_async_remote_copy(
            src_ref=meta.at[0], dst_ref=meta.at[slot], send_sem=msend_sem.at[slot], recv_sem=mrecv_sem.at[slot],
            device_id={'seg': dev}, device_id_type=MESH)
        for slot, dev in peers]
    for copy in metas:
        copy.start()
    columns = {1: reach - 2, 2: reach + 2, 3: reach - 1 - 2 * core, 4: reach + 3 - 2 * core, 5: 2 * reach * core,
               6: reach + 1 - 2 * core}

    def start_rest(k, _):
        to_right(k).start()
        to_left(k).start()
        to_mate(k).start()
        return 0

    lax.fori_loop(1, CHUNKS, start_rest, 0)

    meta[7] = jnp.zeros((2, n), jnp.float32)
    row_id = lax.broadcasted_iota(jnp.int32, (TILE, 2 * TILE), 0)
    col_id = lax.broadcasted_iota(jnp.int32, (TILE, 2 * TILE), 1)
    for half in range(2):
        diag[half] = jnp.where(row_id + half * TILE == col_id, -1e30, 0.0)
    diag[2] = jnp.zeros((TILE, 2 * TILE), jnp.float32)

    def serve(k):
        to_right(k).wait_recv()
        to_left(k).wait_recv()
        pass_left_block(k).start()
        pass_right_block(k).start()
        pass_far(k).start()

    tiles = n // TILE
    ring = 2 * CHUNKS
    last = ring + 4 * CHUNKS

    def place(task):
        turn = task - ring
        slot = jnp.where(task < CHUNKS, 0, jnp.where(task < ring, 6, jnp.where(task < last, 1 + lax.rem(turn, 4), 5)))
        k = jnp.where(task < CHUNKS, CHUNKS - 1 - task,
                      jnp.where(task < ring, task - CHUNKS, jnp.where(task < last, turn // 4, task - last)))
        return slot, k

    def block(slot, k):
        return x_all[slot, pl.ds(pl.multiple_of(k * chunk, chunk), chunk), :]

    def dots(i, slot, k):
        return lax.dot_general(x_all[0, i * TILE:(i + 1) * TILE, :], block(slot, k), (((1,), (1,)), ((), ())),
                               preferred_element_type=jnp.float32)

    def weigh(dot_tile, i, slot, k, buf, cap):
        for p in range(TILE // PIECE):
            rows = slice(i * TILE + p * PIECE, i * TILE + (p + 1) * PIECE)
            tile_rows = slice(p * PIECE, (p + 1) * PIECE)
            a_piece = a_col[rows, :]
            q_piece = q_col[rows, :]
            part = row_acc[rows, :]
            for h in range(chunk // LANES):
                lanes = slice(h * LANES, (h + 1) * LANES)
                cols = pl.ds(pl.multiple_of(k * chunk + h * LANES, LANES), LANES)
                power = (dot_tile[tile_rows, lanes] * (2.0 * scale) + a_piece) + meta[slot, 1:2, cols]
                power = jnp.minimum(power, 0.0 if cap is None else diag[cap, tile_rows, lanes])
                w = jnp.exp2(power) * meta[slot, 0:1, cols] * q_piece
                part = part + w
                w_buf[buf, tile_rows, lanes] = w.astype(jnp.bfloat16)
            row_acc[rows, :] = part

    def pull(i, slot, k, buf):
        acc[i * TILE:(i + 1) * TILE, :] += jnp.dot(w_buf[buf], block(slot, k), preferred_element_type=jnp.float32)

    def run_task(task, own):
        slot, k = place(task)
        was_slot, was_k = place(jnp.maximum(task - 1, 0))
        was_meta = jnp.where(task == 0, 7, was_slot)
        held = s_buf[...]
        for i in range(tiles):
            i1, slot1, k1, meta1 = (tiles - 1, was_slot, was_k, was_meta) if i == 0 else (i - 1, slot, k, slot)
            cap = None
            if own:
                step = i1 - 2 * k1
                cap = jnp.where((step == 0) | (step == 1), step, 2)
            fresh = dots(i, slot, k)
            weigh(held, i1, meta1, k1, i % 2, cap)
            pull(i1, slot1, k1, i % 2)
            held = fresh
        s_buf[...] = held

    s_buf[...] = jnp.zeros(s_buf.shape, jnp.float32)

    def own_tasks(pair, _):
        @pl.when(2 * pair == CHUNKS - 2)
        def _():
            for copy in metas:
                copy.wait_recv()
            for s, column in columns.items():
                meta[s, 0:1, :] = jnp.where(band_ref[0, column] != 0, meta[s, 0:1, :], 0.0)

            def wait_mate(k, _):
                to_mate(k).wait_recv()
                return 0

            lax.fori_loop(0, CHUNKS, wait_mate, 0)
            serve(0)

        run_task(2 * pair, True)
        run_task(2 * pair + 1, True)
        return 0

    lax.fori_loop(0, CHUNKS // 2, own_tasks, 0)

    def arrivals(task):
        coming = task + 1 - ring
        k = coming // 4

        @pl.when((coming >= 0) & (lax.rem(coming, 4) == 0) & (k < CHUNKS))
        def _():
            pass_left_block(k).wait_recv()
            pass_right_block(k).wait_recv()

            @pl.when(k + 1 < CHUNKS)
            def _():
                serve(k + 1)

        @pl.when((task + 1 >= last) & (task + 1 < last + CHUNKS))
        def _():
            pass_far(task + 1 - last).wait_recv()

    def other_tasks(pair, _):
        task = 2 * pair
        arrivals(task)
        arrivals(task + 1)
        run_task(task, False)
        run_task(task + 1, False)
        return 0

    lax.fori_loop(CHUNKS // 2, (last + CHUNKS) // 2, other_tasks, 0)

    slot, k = place(last + CHUNKS - 1)
    weigh(s_buf[...], tiles - 1, slot, k, 0, None)
    pull(tiles - 1, slot, k, 0)

    total = jnp.zeros((8, LANES), jnp.float32)

    def add_rows(r, total):
        rows = pl.ds(pl.multiple_of(r * LANES, LANES), LANES)
        return total + jnp.sum(row_acc[rows, :].reshape(LANES // 8, 8, LANES), axis=0)

    total = lax.fori_loop(0, n // LANES, add_rows, total)
    e_buf[me] = jnp.broadcast_to(0.5 * jnp.sum(total), (8, LANES))

    def finish(r, _):
        rows = pl.ds(pl.multiple_of(r * LANES, LANES), LANES)
        row_sum = jnp.sum(row_acc[rows, :], axis=1, keepdims=True)
        acc[rows, :] = (row_sum * x_all[0, rows, :].astype(jnp.float32) - acc[rows, :]) * inv_lsq
        return 0

    def out_copy(r):
        rows = pl.ds(pl.multiple_of(r * LANES, LANES), LANES)
        return pltpu.make_async_copy(acc.at[rows], f_hbm.at[rows], out_sem.at[r])

    finish(0, 0)
    energy = [
        pltpu.make_async_remote_copy(
            src_ref=e_buf.at[me], dst_ref=e_buf.at[me], send_sem=esend_sem.at[hop], recv_sem=erecv_sem.at[hop],
            device_id={'seg': lax.rem(me + hop, seg_len)}, device_id_type=MESH)
        for hop in range(1, seg_len)]
    for copy in energy:
        copy.start()

    def finish_and_send(r, _):
        finish(r, 0)
        out_copy(r - 1).start()
        return 0

    lax.fori_loop(1, n // LANES, finish_and_send, 0)
    out_copy(n // LANES - 1).start()

    def drain(k, _):
        for copy in (to_right, to_left, to_mate, pass_left_block, pass_right_block, pass_far):
            copy(k).wait_send()
        return 0

    lax.fori_loop(0, CHUNKS, drain, 0)
    for copy in metas:
        copy.wait_send()
    for copy in energy:
        copy.wait()
    e_sum = e_buf[0]
    for dev in range(1, seg_len):
        e_sum = e_sum + e_buf[dev]
    e_ref[0, 0] = e_sum[0, 0]

    def drain_out(r, _):
        out_copy(r).wait()
        return 0

    lax.fori_loop(0, n // LANES, drain_out, 0)


def solution(mesh):
    seg_len = mesh.shape['seg']

    def device_fn(positions, charges, pair_band):
        n, d = positions.shape
        reach = (pair_band.shape[1] - 1) // 2
        flops = 4 * n * n * d * (2 * reach + 1)
        forces, energy = pl.pallas_call(
            functools.partial(kernel, seg_len, reach),
            out_shape=(jax.ShapeDtypeStruct((n, d), jnp.float32), jax.ShapeDtypeStruct((1, 1), jnp.float32)),
            in_specs=[pl.BlockSpec(memory_space=pltpu.SMEM), pl.BlockSpec(memory_space=pl.ANY),
                      pl.BlockSpec(memory_space=pltpu.VMEM)],
            out_specs=(pl.BlockSpec(memory_space=pl.ANY), pl.BlockSpec(memory_space=pltpu.SMEM)),
            scratch_shapes=[
                pltpu.VMEM((7, n, d), jnp.bfloat16),
                pltpu.VMEM((8, 2, n), jnp.float32),
                pltpu.VMEM((n, LANES), jnp.float32),
                pltpu.VMEM((n, LANES), jnp.float32),
                pltpu.VMEM((n, d), jnp.float32),
                pltpu.VMEM((n, LANES), jnp.float32),
                pltpu.VMEM((TILE, 2 * TILE), jnp.float32),
                pltpu.VMEM((2, TILE, 2 * TILE), jnp.bfloat16),
                pltpu.VMEM((3, TILE, 2 * TILE), jnp.float32),
                pltpu.VMEM((seg_len, 8, LANES), jnp.float32),
                pltpu.SemaphoreType.DMA,
                pltpu.SemaphoreType.DMA((6, CHUNKS)),
                pltpu.SemaphoreType.DMA((7, CHUNKS)),
                pltpu.SemaphoreType.DMA((7,)),
                pltpu.SemaphoreType.DMA((7,)),
                pltpu.SemaphoreType.DMA((seg_len,)),
                pltpu.SemaphoreType.DMA((seg_len,)),
                pltpu.SemaphoreType.DMA((n // LANES,)),
            ],
            compiler_params=pltpu.CompilerParams(
                collective_id=0, has_side_effects=True, vmem_limit_bytes=60 * 2**20),
            cost_estimate=pl.CostEstimate(flops=flops, bytes_accessed=16 * n * d, transcendentals=0),
            name='pair_forces',
        )(pair_band, positions, charges.reshape(1, n))
        return forces, energy.reshape(1)

    row_spec = P(('sys', 'seg'), None)
    vec_spec = P(('sys', 'seg'))
    return jax.shard_map(device_fn, mesh=mesh, in_specs=(row_spec, vec_spec, row_spec), out_specs=(row_spec, P('sys')), check_vma=False)
```
